32 devices in a mesh: ta: 1, gx: 8 (over y, x, core), gy: 4 (over z).
Axes of the slice: x: 2, y: 2, z: 4, core: 2. Of those that a mesh axis runs over, the one named last changes fastest.
Arguments:
- propagator: bfloat16 [1, 2, 4, 3, 4, 3, 64, 4096], P('ta', None, None, None, None, None, 'gx', 'gy'), may hold values from -1.5 to 1.5
- gamma_table: int32 [16, 8], replicated, may hold values from 0 to 3, as said below
Outputs:
- spectrum: float32 [1, 16, 64, 64, 128], P('ta', None, ('gx', 'gy'))
The draws below stay inside these ranges and needn't reach their ends.
Inputs may be any that keep to these rules, and one draw needn't show every extreme that they name: gamma_table[g, 0:4] is a permutation of 0 to 3, gamma_table[g, 4:8] are powers of i.
All inputs are finite; a program needn't handle non-finite values.
Results may differ from the reference program's by a relative error of at most 0.0061.
Values may be sent and summed in bfloat16 or wider, within the bound.
A program may use at most 192 MiB of HBM per device.

```python
import math
import jax
import jax.numpy as jnp
from jax import lax

EXTENT = 64
CHANNELS = 16
SLICES = 1


def draw_gamma_table(key, part):
    subkeys = jax.random.split(key, CHANNELS)
    orders = jax.vmap(lambda subkey: jax.random.permutation(subkey, 4))(subkeys)
    phase_codes = jax.random.randint(jax.random.fold_in(key, 11), (CHANNELS, 4), 0, 4, dtype=jnp.int32)
    return jnp.concatenate([orders.astype(jnp.int32), phase_codes], axis=1)


def level_of(stream_key, extent, cuts, low, high):
    factor_of, own = 1.0, jax.random.fold_in(stream_key, 6)
    for position, blocks in cuts:
        steps = jnp.exp(jax.random.uniform(jax.random.fold_in(own, position), (blocks,), jnp.float32, low / len(cuts), high / len(cuts)))
        factor_of = factor_of * jnp.repeat(steps, extent[position] // blocks).reshape([-1 if axis == position else 1 for axis in range(len(extent))])
    return factor_of


def bell_draw(key, shape, deviation, reach, pieces=(), kind=jnp.bfloat16):
    factor_of = level_of(key, shape, pieces, -0.22, 0.18) if pieces else 1.0
    array = jax.random.normal(key, shape, jnp.float32) * deviation * factor_of
    return jnp.minimum(jnp.maximum(array, -reach), reach).astype(kind)


def setup_inputs(seed: int = 0) -> dict:
    key_of = jax.random.split(jax.random.key(seed), 3)
    propagator = bell_draw(key_of[0], (SLICES, 2, 4, 3, 4, 3, EXTENT, EXTENT * EXTENT), 0.25, 1.5, ((6, 8), (7, 4)))
    gamma_table = draw_gamma_table(jax.random.fold_in(key_of[2], 71), 0)
    return dict(propagator=propagator, gamma_table=gamma_table)


def precise_dot(left_matrix, right_matrix):
    return jnp.dot(left_matrix, right_matrix, precision=lax.Precision.HIGHEST, preferred_element_type=jnp.float32)

def channel_weights(channel_table):
    spin_index = jnp.arange(4, dtype=jnp.int32)
    targets = channel_table[:, :4]
    codes_all = channel_table[:, 4:]
    mapping = (targets[:, :, None] == spin_index[None, None, :]).astype(jnp.float32)
    phase_real = (codes_all == 0).astype(jnp.float32) - (codes_all == 2).astype(jnp.float32)
    phase_imag = (codes_all == 1).astype(jnp.float32) - (codes_all == 3).astype(jnp.float32)
    pair_real = phase_real[:, None, :] * phase_real[:, :, None] - phase_imag[:, None, :] * phase_imag[:, :, None]
    pair_imag = phase_real[:, None, :] * phase_imag[:, :, None] + phase_imag[:, None, :] * phase_real[:, :, None]
    source_map = jnp.transpose(mapping, (0, 2, 1))
    selector = source_map[:, :, None, :, None] * mapping[:, None, :, None, :]
    count_channels = channel_table.shape[0]
    weight_real = (pair_real[:, None, :, :, None] * selector).reshape(count_channels, 256)
    weight_imag = (pair_imag[:, None, :, :, None] * selector).reshape(count_channels, 256)
    return (weight_real, weight_imag)

def spin_products(field_real, field_imag):
    site_count = field_real.shape[-1]
    total_real = jnp.zeros((4, 4, 4, 4, site_count), jnp.float32)
    total_imag = jnp.zeros((4, 4, 4, 4, site_count), jnp.float32)
    for color_in in range(3):
        for color_out in range(3):
            left_real = field_real[:, color_in, :, color_out].astype(jnp.float32)
            left_imag = field_imag[:, color_in, :, color_out].astype(jnp.float32)
            total_real = total_real + left_real[:, :, None, None] * left_real[None, None] + left_imag[:, :, None, None] * left_imag[None, None]
            total_imag = total_imag + left_imag[:, :, None, None] * left_real[None, None] - left_real[:, :, None, None] * left_imag[None, None]
    return (total_real.reshape(256, site_count), total_imag.reshape(256, site_count))

def dft_tables(length):
    steps_index = jnp.arange(length, dtype=jnp.int32)
    phases = steps_index[:, None] * steps_index[None, :] % length
    angles = phases.astype(jnp.float32) * (2.0 * math.pi / length)
    norm_factor = 1.0 / math.sqrt(length)
    cosine = (jnp.cos(angles) * norm_factor).astype(jnp.bfloat16)
    sine_table = (jnp.sin(angles) * norm_factor).astype(jnp.bfloat16)
    return (cosine.astype(jnp.float32), sine_table.astype(jnp.float32))

def section(complex_pair, which_axis, cosine, sine_table):
    field_real = complex_pair[0].astype(jnp.float32)
    field_imag = complex_pair[1].astype(jnp.float32)

    def contract_axis(values, weights):
        moved = jnp.tensordot(values, weights, axes=([which_axis], [0]), precision=lax.Precision.HIGHEST)
        return jnp.moveaxis(moved, -1, which_axis)
    new_real = contract_axis(field_real, cosine) + contract_axis(field_imag, sine_table)
    new_imag = contract_axis(field_imag, cosine) - contract_axis(field_real, sine_table)
    return (new_real, new_imag)

def to_half(complex_pair):
    return lax.optimization_barrier((complex_pair[0].astype(jnp.bfloat16), complex_pair[1].astype(jnp.bfloat16)))

def reference(propagator, gamma_table):
    weight_real, weight_imag = channel_weights(gamma_table)
    stack_real = jnp.concatenate([weight_real, -weight_imag], axis=1)
    stack_imag = jnp.concatenate([weight_imag, weight_real], axis=1)
    cosine, sine_table = dft_tables(EXTENT)
    volume = EXTENT ** 3

    def one_slice(slice_block):
        flattened = slice_block.astype(jnp.float32).reshape(2, 4, 3, 4, 3, volume)
        prod_real, prod_imag = spin_products(flattened[0], flattened[1])
        prod_stack = jnp.concatenate([prod_real, prod_imag], axis=0).astype(jnp.bfloat16)
        prod_stack = lax.optimization_barrier(prod_stack).astype(jnp.float32)
        dens_real = precise_dot(stack_real, prod_stack).reshape(-1, EXTENT, EXTENT, EXTENT)
        dens_imag = precise_dot(stack_imag, prod_stack).reshape(-1, EXTENT, EXTENT, EXTENT)
        pair = to_half((dens_real, dens_imag))
        pair = to_half(section(pair, 3, cosine, sine_table))
        pair = to_half(section(pair, 2, cosine, sine_table))
        spec_real, spec_imag = section(pair, 1, cosine, sine_table)
        spec_real = jnp.transpose(spec_real, (0, 3, 1, 2))
        spec_imag = jnp.transpose(spec_imag, (0, 3, 1, 2))
        return jnp.concatenate([spec_real, spec_imag], axis=3).astype(jnp.float32)
    return lax.map(one_slice, propagator)
```

```python
import functools
import math

import jax
import jax.numpy as jnp
import numpy as np
from jax import lax
from jax.experimental import pallas as pl
from jax.experimental.pallas import tpu as pltpu
from jax.sharding import PartitionSpec as P

REMOTE = False
LANES = 128
SPINS = 4
COLORS = 3
PAIRED = 2
MESH = pl.DeviceIdType.MESH


def pair_rows():
    rows = []
    for left in range(SPINS):
        for right in range(left, SPINS):
            for i in range(SPINS):
                for j in range(SPINS):
                    if left == right and i > j:
                        continue
                    if left == right and i == j:
                        rows.append((left, i, right, j, 2))
                    else:
                        rows.append((left, i, right, j, 0))
                        rows.append((left, i, right, j, 1))
    return rows


ROWS = pair_rows()
ROW_OF = {row: position for position, row in enumerate(ROWS)}


def dft_tables(length):
    index = np.arange(length)
    angles = (index[:, None] * index[None, :] % length) * (2.0 * math.pi / length)
    norm = 1.0 / math.sqrt(length)
    half = lambda v: (v * norm).astype(jnp.bfloat16).astype(np.float32)
    return half(np.cos(angles)), half(np.sin(angles))


def table_z(extent):
    cosine, sine = dft_tables(extent)
    per_tile = LANES // extent
    same = np.eye(per_tile, dtype=np.float32)
    block = np.zeros((extent, 2, per_tile, 2, per_tile, extent), np.float32)
    for c_out, c_in, values in ((0, 0, cosine), (0, 1, sine), (1, 0, -sine), (1, 1, cosine)):
        block[:, c_out, :, c_in] = np.einsum("zk,ab->kabz", values, same)
    return block.reshape(2 * LANES, 2 * LANES)


def table_y(extent, local_k):
    cosine, sine = dft_tables(extent)
    per_tile = LANES // extent
    groups = extent // per_tile
    block = np.zeros((groups, local_k, 2, per_tile, 2, local_k, 2, extent), np.float32)
    entries = (
        (0, 0, 0, cosine), (0, 0, 1, sine), (0, 1, 0, -sine), (0, 1, 1, cosine),
        (1, 0, 0, -sine), (1, 0, 1, cosine), (1, 1, 0, -cosine), (1, 1, 1, -sine),
    )
    for copy, c_out, c_in, values in entries:
        for k in range(local_k):
            block[:, k, c_in, :, copy, k, c_out] = values.reshape(groups, per_tile, extent)
    return block.reshape(groups * local_k * 2 * per_tile, 2 * local_k * 2 * extent)


def table_x(extent):
    cosine, sine = dft_tables(extent)
    return np.concatenate([cosine.T, sine.T], axis=1)


def folded_weights(table, rows):
    channels = table.shape[0]
    a1, a2, b1, b2, kind = (rows[i : i + 1, :] for i in range(5))

    def pick(spin, base):
        value = jnp.zeros((channels, rows.shape[1]), jnp.int32)
        for s in range(SPINS):
            value = jnp.where(spin == s, table[:, base + s : base + s + 1], value)
        return value

    def term(l1, l2, r1, r2):
        hit = (pick(r1, 0) == l1) & (pick(l2, 0) == r2)
        code = (pick(r1, SPINS) + pick(l2, SPINS)) & 3
        one = jnp.where(hit, 1.0, 0.0)
        real = jnp.where(code == 0, one, jnp.where(code == 2, -one, 0.0))
        imag = jnp.where(code == 1, one, jnp.where(code == 3, -one, 0.0))
        return real, imag

    fore_real, fore_imag = term(a1, a2, b1, b2)
    back_real, back_imag = term(b1, b2, a1, a2)
    sign = jnp.where(kind == 0, 1.0, jnp.where(kind == 1, -1.0, 0.0))
    real = fore_real + sign * back_real
    imag = fore_imag + sign * back_imag
    weight_real = jnp.where(kind == 1, -imag, real)
    weight_imag = jnp.where(kind == 1, real, imag)
    return jnp.concatenate([weight_real, weight_imag], axis=0).astype(jnp.bfloat16)


def component(s1, c1, s2, c2):
    return ((s1 * COLORS + c1) * SPINS + s2) * COLORS + c2


def products(parts, rows_out):
    def put(row, value):
        rows_out[pl.ds(ROW_OF[row] * 8, 8), :] = value

    colors = [(c1, c2) for c1 in range(COLORS) for c2 in range(COLORS)]
    for left in range(SPINS):
        for right in range(left, SPINS):
            for half in ((0, 1), (2, 3)):
                pairs = [(i, j) for i in half for j in range(SPINS) if left != right or i < j]
                diagonal = half if left == right else ()
                sums = {}
                for c1, c2 in colors:
                    at_a = {i: component(left, c1, i, c2) for i in half}
                    at_b = {j: component(right, c1, j, c2) for j in {j for _, j in pairs}}
                    a = {i: (parts[0, n], parts[1, n], parts[2, n]) for i, n in at_a.items()}
                    b = {j: (parts[0, n], parts[2, n], parts[3, n]) for j, n in at_b.items()}
                    for i, j in pairs:
                        new = (a[i][2] * b[j][0], a[i][0] * b[j][1], a[i][1] * b[j][2])
                        old = sums.get((i, j))
                        sums[i, j] = new if old is None else tuple(o + v for o, v in zip(old, new))
                    for i in diagonal:
                        new = a[i][0] * a[i][0] + a[i][1] * a[i][1]
                        old = sums.get(i)
                        sums[i] = new if old is None else old + new
                for i, j in pairs:
                    first, second, third = sums[i, j]
                    put((left, i, right, j, 0), first - third)
                    put((left, i, right, j, 1), first - second)
                for i in diagonal:
                    put((left, i, right, i, 2), sums[i])


def front_kernel(
    remote, grid_y, prop, table, rows, dft, out,
    staged, parts, prod, dens, weights, sent, load_sems, send_sem, recv_sem,
):
    devices, steps = out.shape[0], out.shape[1]
    tiles = staged.shape[0]
    entries = parts.shape[1]
    channels = table.shape[0]

    def load(t):
        return pltpu.make_async_copy(
            prop.at[:, :, pl.ds(t * LANES, LANES)], staged.at[t], load_sems.at[t]
        )

    for t in range(tiles):
        load(t).start()
    if remote:
        me_x, me_y = lax.axis_index("gx"), lax.axis_index("gy")
        me = me_x * grid_y + me_y
        barrier = pltpu.get_barrier_semaphore()

        @pl.loop(1, devices)
        def _(i):
            to = lax.rem(me + i, devices)
            pl.semaphore_signal(
                barrier, inc=1, device_id={"gx": to // grid_y, "gy": lax.rem(to, grid_y)},
                device_id_type=MESH,
            )

    weights[...] = folded_weights(table[...], rows[...])
    if remote:
        pl.semaphore_wait(barrier, devices - 1)

    @pl.loop(0, steps)
    def _(k):
        @pl.loop(0, PAIRED)
        def _(half):
            t = k * PAIRED + half
            pltpu.make_async_copy(
                prop.at[:, :, pl.ds(0, LANES)], staged.at[t], load_sems.at[t]
            ).wait()
            real = staged[t, 0:entries].astype(jnp.float32)
            parts[0] = real
            imag = staged[t, entries : 2 * entries].astype(jnp.float32)
            parts[1] = imag
            parts[2] = real + imag
            parts[3] = real - imag
            products(parts, prod)
            for x in range(8):
                columns = prod[pl.ds(x, len(ROWS), stride=8), :].astype(jnp.bfloat16)
                value = jnp.dot(weights[...], columns, preferred_element_type=jnp.float32)
                dens[half, 0, pl.ds(x, channels, stride=8), :] = value[:channels]
                dens[half, 1, pl.ds(x, channels, stride=8), :] = value[channels:]

        pieces = []
        for half in range(PAIRED):
            left = jnp.concatenate([dens[half, 0], dens[half, 1]], axis=1).astype(jnp.bfloat16)
            value = lax.dot_general(
                dft[...], left, (((1,), (1,)), ((), ())), preferred_element_type=jnp.float32
            )
            pieces.append(value.reshape(devices, 2 * LANES // devices, LANES))
        block = jnp.concatenate(pieces, axis=1).astype(jnp.bfloat16)
        if not remote:
            out[:, k] = block
        else:
            sent[:, k] = block
            pltpu.make_async_copy(sent.at[me, k], out.at[me, k], recv_sem).start()

            @pl.loop(1, devices)
            def _(i):
                to = lax.rem(me + i, devices)
                pltpu.make_async_remote_copy(
                    src_ref=sent.at[to, k], dst_ref=out.at[me, k],
                    send_sem=send_sem, recv_sem=recv_sem,
                    device_id={"gx": to // grid_y, "gy": lax.rem(to, grid_y)},
                    device_id_type=MESH,
                ).start()

    if remote:
        pltpu.make_async_copy(out, out, recv_sem).wait()
        rest = sent.at[pl.ds(0, devices - 1)]
        pltpu.make_async_copy(rest, rest, send_sem).wait()


def front(prop, gamma_table, devices, grid_y, extent):
    entries, rows_x, sites = prop.shape
    tiles = sites // LANES
    steps = tiles // PAIRED
    height = 2 * LANES // devices * PAIRED
    channels = gamma_table.shape[0]
    rows = np.zeros((8, len(ROWS)), np.int32)
    rows[:5] = np.array(ROWS, np.int32).T
    vmem = pl.BlockSpec(memory_space=pltpu.VMEM)
    return pl.pallas_call(
        functools.partial(front_kernel, REMOTE, grid_y),
        out_shape=jax.ShapeDtypeStruct((devices, steps, height, LANES), jnp.bfloat16),
        in_specs=[pl.BlockSpec(memory_space=pl.ANY), vmem, vmem, vmem],
        out_specs=pl.BlockSpec(memory_space=pl.ANY) if REMOTE else vmem,
        scratch_shapes=[
            pltpu.VMEM((tiles, entries, rows_x, LANES), jnp.bfloat16),
            pltpu.VMEM((4, entries // 2, rows_x, LANES), jnp.float32),
            pltpu.VMEM((len(ROWS) * rows_x, LANES), jnp.float32),
            pltpu.VMEM((PAIRED, 2, channels * rows_x, LANES), jnp.float32),
            pltpu.VMEM((2 * channels, len(ROWS)), jnp.bfloat16),
            pltpu.VMEM((devices, steps, height, LANES), jnp.bfloat16),
            pltpu.SemaphoreType.DMA((tiles,)),
            pltpu.SemaphoreType.DMA,
            pltpu.SemaphoreType.DMA,
        ],
        compiler_params=pltpu.CompilerParams(
            vmem_limit_bytes=40 * 1024 * 1024,
            **(dict(collective_id=0, has_side_effects=True) if REMOTE else {}),
        ),
    )(prop, gamma_table, jnp.asarray(rows), jnp.asarray(table_z(extent), jnp.bfloat16))


def back_kernel(blocks, along_y, along_x, out, mid):
    grid_x, _, width = blocks.shape
    channels, local_k, extent, lanes = out.shape
    rows_x = width // channels
    cols = local_k * lanes
    for gx in range(grid_x):
        mid[gx] = lax.dot_general(
            blocks[gx], along_y[...], (((0,), (0,)), ((), ())), preferred_element_type=jnp.float32
        )
    for g in range(channels):
        value = mid[:, g * rows_x : (g + 1) * rows_x, :].reshape(grid_x * rows_x, 2 * cols)
        value = value.astype(jnp.bfloat16)
        stacked = jnp.concatenate([value[:, :cols], value[:, cols:]], axis=0)
        result = jnp.dot(along_x[...], stacked, preferred_element_type=jnp.float32)
        for k in range(local_k):
            out[g, k] = result[:, k * lanes : (k + 1) * lanes]


def back(blocks, channels, extent, local_k):
    grid_x, _, width = blocks.shape
    vmem = pl.BlockSpec(memory_space=pltpu.VMEM)
    return pl.pallas_call(
        back_kernel,
        out_shape=jax.ShapeDtypeStruct((channels, local_k, extent, 2 * extent), jnp.float32),
        in_specs=[vmem] * 3,
        out_specs=vmem,
        scratch_shapes=[pltpu.VMEM((grid_x, width, 4 * local_k * extent), jnp.float32)],
        compiler_params=pltpu.CompilerParams(vmem_limit_bytes=24 * 1024 * 1024),
    )(
        blocks,
        jnp.asarray(table_y(extent, local_k), jnp.bfloat16),
        jnp.asarray(table_x(extent), jnp.bfloat16),
    )


def body(propagator, gamma_table):
    slices, rows_x, sites = propagator.shape[0], propagator.shape[-2], propagator.shape[-1]
    grid_x, grid_y = lax.axis_size("gx"), lax.axis_size("gy")
    devices = grid_x * grid_y
    extent = grid_x * rows_x
    channels = gamma_table.shape[0]
    local_k = extent // devices
    results = []
    for t in range(slices):
        prop = propagator[t].reshape(-1, rows_x, sites)
        blocks = front(prop, gamma_table, devices, grid_y, extent)
        if not REMOTE:
            blocks = lax.all_to_all(blocks, ("gx", "gy"), split_axis=0, concat_axis=0, tiled=True)
        blocks = blocks.reshape(grid_x, -1, LANES)
        results.append(back(blocks, channels, extent, local_k))
    return jnp.stack(results)


def solution(mesh):
    return jax.shard_map(
        body,
        mesh=mesh,
        in_specs=(P("ta", None, None, None, None, None, "gx", "gy"), P()),
        out_specs=P("ta", None, ("gx", "gy"), None, None),
        check_vma=False,
    )
```

```python
import functools
import math

import jax
import jax.numpy as jnp
import numpy as np
from jax import lax
from jax.experimental import pallas as pl
from jax.experimental.pallas import tpu as pltpu
from jax.sharding import PartitionSpec as P

REMOTE = True
LANES = 128
SPINS = 4
COLORS = 3
PAIRED = 2
MESH = pl.DeviceIdType.MESH


def pair_rows():
    rows = []
    for left in range(SPINS):
        for right in range(left, SPINS):
            for i in range(SPINS):
                for j in range(SPINS):
                    if left == right and i > j:
                        continue
                    if left == right and i == j:
                        rows.append((left, i, right, j, 2))
                    else:
                        rows.append((left, i, right, j, 0))
                        rows.append((left, i, right, j, 1))
    return rows


ROWS = pair_rows()
ROW_OF = {row: position for position, row in enumerate(ROWS)}


def dft_tables(length):
    index = np.arange(length)
    angles = (index[:, None] * index[None, :] % length) * (2.0 * math.pi / length)
    norm = 1.0 / math.sqrt(length)
    half = lambda v: (v * norm).astype(jnp.bfloat16).astype(np.float32)
    return half(np.cos(angles)), half(np.sin(angles))


def table_z(extent):
    cosine, sine = dft_tables(extent)
    per_tile = LANES // extent
    same = np.eye(per_tile, dtype=np.float32)
    block = np.zeros((extent, 2, per_tile, 2, per_tile, extent), np.float32)
    for c_out, c_in, values in ((0, 0, cosine), (0, 1, sine), (1, 0, -sine), (1, 1, cosine)):
        block[:, c_out, :, c_in] = np.einsum("zk,ab->kabz", values, same)
    return block.reshape(2 * LANES, 2 * LANES)


def table_y(extent, local_k):
    cosine, sine = dft_tables(extent)
    per_tile = LANES // extent
    groups = extent // per_tile
    block = np.zeros((groups, local_k, 2, per_tile, 2, local_k, 2, extent), np.float32)
    entries = (
        (0, 0, 0, cosine), (0, 0, 1, sine), (0, 1, 0, -sine), (0, 1, 1, cosine),
        (1, 0, 0, -sine), (1, 0, 1, cosine), (1, 1, 0, -cosine), (1, 1, 1, -sine),
    )
    for copy, c_out, c_in, values in entries:
        for k in range(local_k):
            block[:, k, c_in, :, copy, k, c_out] = values.reshape(groups, per_tile, extent)
    return block.reshape(groups * local_k * 2 * per_tile, 2 * local_k * 2 * extent)


def table_x(extent):
    cosine, sine = dft_tables(extent)
    return np.concatenate([cosine.T, sine.T], axis=1)


def folded_weights(table, rows):
    channels = table.shape[0]
    a1, a2, b1, b2, kind = (rows[i : i + 1, :] for i in range(5))

    def pick(spin, base):
        value = jnp.zeros((channels, rows.shape[1]), jnp.int32)
        for s in range(SPINS):
            value = jnp.where(spin == s, table[:, base + s : base + s + 1], value)
        return value

    def term(l1, l2, r1, r2):
        hit = (pick(r1, 0) == l1) & (pick(l2, 0) == r2)
        code = (pick(r1, SPINS) + pick(l2, SPINS)) & 3
        one = jnp.where(hit, 1.0, 0.0)
        real = jnp.where(code == 0, one, jnp.where(code == 2, -one, 0.0))
        imag = jnp.where(code == 1, one, jnp.where(code == 3, -one, 0.0))
        return real, imag

    fore_real, fore_imag = term(a1, a2, b1, b2)
    back_real, back_imag = term(b1, b2, a1, a2)
    sign = jnp.where(kind == 0, 1.0, jnp.where(kind == 1, -1.0, 0.0))
    real = fore_real + sign * back_real
    imag = fore_imag + sign * back_imag
    weight_real = jnp.where(kind == 1, -imag, real)
    weight_imag = jnp.where(kind == 1, real, imag)
    return jnp.concatenate([weight_real, weight_imag], axis=0).astype(jnp.bfloat16)


def component(s1, c1, s2, c2):
    return ((s1 * COLORS + c1) * SPINS + s2) * COLORS + c2


def products(parts, rows_out):
    def put(row, value):
        rows_out[pl.ds(ROW_OF[row] * 8, 8), :] = value

    colors = [(c1, c2) for c1 in range(COLORS) for c2 in range(COLORS)]
    for left in range(SPINS):
        for right in range(left, SPINS):
            for half in ((0, 1), (2, 3)):
                pairs = [(i, j) for i in half for j in range(SPINS) if left != right or i < j]
                diagonal = half if left == right else ()
                sums = {}
                for c1, c2 in colors:
                    at_a = {i: component(left, c1, i, c2) for i in half}
                    at_b = {j: component(right, c1, j, c2) for j in {j for _, j in pairs}}
                    a = {i: (parts[0, n], parts[1, n], parts[2, n]) for i, n in at_a.items()}
                    b = {j: (parts[0, n], parts[2, n], parts[3, n]) for j, n in at_b.items()}
                    for i, j in pairs:
                        new = (a[i][2] * b[j][0], a[i][0] * b[j][1], a[i][1] * b[j][2])
                        old = sums.get((i, j))
                        sums[i, j] = new if old is None else tuple(o + v for o, v in zip(old, new))
                    for i in diagonal:
                        new = a[i][0] * a[i][0] + a[i][1] * a[i][1]
                        old = sums.get(i)
                        sums[i] = new if old is None else old + new
                for i, j in pairs:
                    first, second, third = sums[i, j]
                    put((left, i, right, j, 0), first - third)
                    put((left, i, right, j, 1), first - second)
                for i in diagonal:
                    put((left, i, right, i, 2), sums[i])


def front_kernel(
    remote, grid_y, prop, table, rows, dft, out,
    staged, parts, prod, dens, weights, sent, load_sems, send_sem, recv_sem,
):
    devices, steps = out.shape[0], out.shape[1]
    tiles = staged.shape[0]
    entries = parts.shape[1]
    channels = table.shape[0]

    def load(t):
        return pltpu.make_async_copy(
            prop.at[:, :, pl.ds(t * LANES, LANES)], staged.at[t], load_sems.at[t]
        )

    for t in range(tiles):
        load(t).start()
    if remote:
        me_x, me_y = lax.axis_index("gx"), lax.axis_index("gy")
        me = me_x * grid_y + me_y
        barrier = pltpu.get_barrier_semaphore()

        @pl.loop(1, devices)
        def _(i):
            to = lax.rem(me + i, devices)
            pl.semaphore_signal(
                barrier, inc=1, device_id={"gx": to // grid_y, "gy": lax.rem(to, grid_y)},
                device_id_type=MESH,
            )

    weights[...] = folded_weights(table[...], rows[...])
    if remote:
        pl.semaphore_wait(barrier, devices - 1)

    @pl.loop(0, steps)
    def _(k):
        @pl.loop(0, PAIRED)
        def _(half):
            t = k * PAIRED + half
            pltpu.make_async_copy(
                prop.at[:, :, pl.ds(0, LANES)], staged.at[t], load_sems.at[t]
            ).wait()
            real = staged[t, 0:entries].astype(jnp.float32)
            parts[0] = real
            imag = staged[t, entries : 2 * entries].astype(jnp.float32)
            parts[1] = imag
            parts[2] = real + imag
            parts[3] = real - imag
            products(parts, prod)
            for x in range(8):
                columns = prod[pl.ds(x, len(ROWS), stride=8), :].astype(jnp.bfloat16)
                value = jnp.dot(weights[...], columns, preferred_element_type=jnp.float32)
                dens[half, 0, pl.ds(x, channels, stride=8), :] = value[:channels]
                dens[half, 1, pl.ds(x, channels, stride=8), :] = value[channels:]

        pieces = []
        for half in range(PAIRED):
            left = jnp.concatenate([dens[half, 0], dens[half, 1]], axis=1).astype(jnp.bfloat16)
            value = lax.dot_general(
                dft[...], left, (((1,), (1,)), ((), ())), preferred_element_type=jnp.float32
            )
            pieces.append(value.reshape(devices, 2 * LANES // devices, LANES))
        block = jnp.concatenate(pieces, axis=1).astype(jnp.bfloat16)
        if not remote:
            out[:, k] = block
        else:
            sent[:, k] = block
            pltpu.make_async_copy(sent.at[me, k], out.at[me, k], recv_sem).start()

            @pl.loop(1, devices)
            def _(i):
                to = lax.rem(me + i, devices)
                pltpu.make_async_remote_copy(
                    src_ref=sent.at[to, k], dst_ref=out.at[me, k],
                    send_sem=send_sem, recv_sem=recv_sem,
                    device_id={"gx": to // grid_y, "gy": lax.rem(to, grid_y)},
                    device_id_type=MESH,
                ).start()

    if remote:
        pltpu.make_async_copy(out, out, recv_sem).wait()
        rest = sent.at[pl.ds(0, devices - 1)]
        pltpu.make_async_copy(rest, rest, send_sem).wait()


def front(prop, gamma_table, devices, grid_y, extent):
    entries, rows_x, sites = prop.shape
    tiles = sites // LANES
    steps = tiles // PAIRED
    height = 2 * LANES // devices * PAIRED
    channels = gamma_table.shape[0]
    rows = np.zeros((8, len(ROWS)), np.int32)
    rows[:5] = np.array(ROWS, np.int32).T
    vmem = pl.BlockSpec(memory_space=pltpu.VMEM)
    return pl.pallas_call(
        functools.partial(front_kernel, REMOTE, grid_y),
        out_shape=jax.ShapeDtypeStruct((devices, steps, height, LANES), jnp.bfloat16),
        in_specs=[pl.BlockSpec(memory_space=pl.ANY), vmem, vmem, vmem],
        out_specs=pl.BlockSpec(memory_space=pl.ANY) if REMOTE else vmem,
        scratch_shapes=[
            pltpu.VMEM((tiles, entries, rows_x, LANES), jnp.bfloat16),
            pltpu.VMEM((4, entries // 2, rows_x, LANES), jnp.float32),
            pltpu.VMEM((len(ROWS) * rows_x, LANES), jnp.float32),
            pltpu.VMEM((PAIRED, 2, channels * rows_x, LANES), jnp.float32),
            pltpu.VMEM((2 * channels, len(ROWS)), jnp.bfloat16),
            pltpu.VMEM((devices, steps, height, LANES), jnp.bfloat16),
            pltpu.SemaphoreType.DMA((tiles,)),
            pltpu.SemaphoreType.DMA,
            pltpu.SemaphoreType.DMA,
        ],
        compiler_params=pltpu.CompilerParams(
            vmem_limit_bytes=62 * 1024 * 1024,
            **(dict(collective_id=0, has_side_effects=True) if REMOTE else {}),
        ),
    )(prop, gamma_table, jnp.asarray(rows), jnp.asarray(table_z(extent), jnp.bfloat16))


def back_kernel(blocks, along_y, along_x, out, mid):
    grid_x, _, width = blocks.shape
    channels, local_k, extent, lanes = out.shape
    rows_x = width // channels
    cols = local_k * lanes
    for gx in range(grid_x):
        mid[gx] = lax.dot_general(
            blocks[gx], along_y[...], (((0,), (0,)), ((), ())), preferred_element_type=jnp.float32
        )
    for g in range(channels):
        value = mid[:, g * rows_x : (g + 1) * rows_x, :].reshape(grid_x * rows_x, 2 * cols)
        value = value.astype(jnp.bfloat16)
        stacked = jnp.concatenate([value[:, :cols], value[:, cols:]], axis=0)
        result = jnp.dot(along_x[...], stacked, preferred_element_type=jnp.float32)
        for k in range(local_k):
            out[g, k] = result[:, k * lanes : (k + 1) * lanes]


def back(blocks, channels, extent, local_k):
    grid_x, _, width = blocks.shape
    vmem = pl.BlockSpec(memory_space=pltpu.VMEM)
    return pl.pallas_call(
        back_kernel,
        out_shape=jax.ShapeDtypeStruct((channels, local_k, extent, 2 * extent), jnp.float32),
        in_specs=[vmem] * 3,
        out_specs=vmem,
        scratch_shapes=[pltpu.VMEM((grid_x, width, 4 * local_k * extent), jnp.float32)],
        compiler_params=pltpu.CompilerParams(vmem_limit_bytes=24 * 1024 * 1024),
    )(
        blocks,
        jnp.asarray(table_y(extent, local_k), jnp.bfloat16),
        jnp.asarray(table_x(extent), jnp.bfloat16),
    )


def body(propagator, gamma_table):
    slices, rows_x, sites = propagator.shape[0], propagator.shape[-2], propagator.shape[-1]
    grid_x, grid_y = lax.axis_size("gx"), lax.axis_size("gy")
    devices = grid_x * grid_y
    extent = grid_x * rows_x
    channels = gamma_table.shape[0]
    local_k = extent // devices
    results = []
    for t in range(slices):
        prop = propagator[t].reshape(-1, rows_x, sites)
        blocks = front(prop, gamma_table, devices, grid_y, extent)
        if not REMOTE:
            blocks = lax.all_to_all(blocks, ("gx", "gy"), split_axis=0, concat_axis=0, tiled=True)
        blocks = blocks.reshape(grid_x, -1, LANES)
        results.append(back(blocks, channels, extent, local_k))
    return jnp.stack(results)


def solution(mesh):
    return jax.shard_map(
        body,
        mesh=mesh,
        in_specs=(P("ta", None, None, None, None, None, "gx", "gy"), P()),
        out_specs=P("ta", None, ("gx", "gy"), None, None),
        check_vma=False,
    )
```

```python
import functools
import math

import jax
import jax.numpy as jnp
import numpy as np
from jax import lax
from jax.experimental import pallas as pl
from jax.experimental.pallas import tpu as pltpu
from jax.sharding import PartitionSpec as P

LANES = 128
SPINS = 4
COLORS = 3
PAIRED = 1
MESH = pl.DeviceIdType.MESH


def pair_rows():
    rows = []
    for left in range(SPINS):
        for right in range(left, SPINS):
            for i in range(SPINS):
                for j in range(SPINS):
                    if left == right and i > j:
                        continue
                    if left == right and i == j:
                        rows.append((left, i, right, j, 2))
                    else:
                        rows.append((left, i, right, j, 0))
                        rows.append((left, i, right, j, 1))
    return rows


ROWS = pair_rows()
ROW_OF = {row: position for position, row in enumerate(ROWS)}


def dft_tables(length):
    index = np.arange(length)
    angles = (index[:, None] * index[None, :] % length) * (2.0 * math.pi / length)
    norm = 1.0 / math.sqrt(length)
    half = lambda v: (v * norm).astype(jnp.bfloat16).astype(np.float32)
    return half(np.cos(angles)), half(np.sin(angles))


def table_z(extent):
    cosine, sine = dft_tables(extent)
    per_tile = LANES // extent
    same = np.eye(per_tile, dtype=np.float32)
    block = np.zeros((extent, 2, per_tile, 2, per_tile, extent), np.float32)
    for c_out, c_in, values in ((0, 0, cosine), (0, 1, sine), (1, 0, -sine), (1, 1, cosine)):
        block[:, c_out, :, c_in] = np.einsum("zk,ab->kabz", values, same)
    return block.reshape(2 * LANES, 2 * LANES)


def table_y(extent, local_k):
    cosine, sine = dft_tables(extent)
    per_tile = LANES // extent
    groups = extent // per_tile
    block = np.zeros((groups, local_k, 2, per_tile, 2, local_k, 2, extent), np.float32)
    entries = (
        (0, 0, 0, cosine), (0, 0, 1, sine), (0, 1, 0, -sine), (0, 1, 1, cosine),
        (1, 0, 0, -sine), (1, 0, 1, cosine), (1, 1, 0, -cosine), (1, 1, 1, -sine),
    )
    for copy, c_out, c_in, values in entries:
        for k in range(local_k):
            block[:, k, c_in, :, copy, k, c_out] = values.reshape(groups, per_tile, extent)
    return block.reshape(groups * local_k * 2 * per_tile, 2 * local_k * 2 * extent)


def table_x(extent):
    cosine, sine = dft_tables(extent)
    return np.concatenate([cosine.T, sine.T], axis=1)


def folded_weights(table, rows):
    channels = table.shape[0]
    a1, a2, b1, b2, kind = (rows[i : i + 1, :] for i in range(5))

    def pick(spin, base):
        value = jnp.zeros((channels, rows.shape[1]), jnp.int32)
        for s in range(SPINS):
            value = jnp.where(spin == s, table[:, base + s : base + s + 1], value)
        return value

    def term(l1, l2, r1, r2):
        hit = (pick(r1, 0) == l1) & (pick(l2, 0) == r2)
        code = (pick(r1, SPINS) + pick(l2, SPINS)) & 3
        one = jnp.where(hit, 1.0, 0.0)
        real = jnp.where(code == 0, one, jnp.where(code == 2, -one, 0.0))
        imag = jnp.where(code == 1, one, jnp.where(code == 3, -one, 0.0))
        return real, imag

    fore_real, fore_imag = term(a1, a2, b1, b2)
    back_real, back_imag = term(b1, b2, a1, a2)
    sign = jnp.where(kind == 0, 1.0, jnp.where(kind == 1, -1.0, 0.0))
    real = fore_real + sign * back_real
    imag = fore_imag + sign * back_imag
    weight_real = jnp.where(kind == 1, -imag, real)
    weight_imag = jnp.where(kind == 1, real, imag)
    return jnp.concatenate([weight_real, weight_imag], axis=0).astype(jnp.bfloat16)


def component(s1, c1, s2, c2):
    return ((s1 * COLORS + c1) * SPINS + s2) * COLORS + c2


def products(parts, rows_out):
    def put(row, value):
        rows_out[pl.ds(ROW_OF[row] * 8, 8), :] = value

    colors = [(c1, c2) for c1 in range(COLORS) for c2 in range(COLORS)]
    for left in range(SPINS):
        for right in range(left, SPINS):
            for half in ((0, 1), (2, 3)):
                pairs = [(i, j) for i in half for j in range(SPINS) if left != right or i < j]
                diagonal = half if left == right else ()
                sums = {}
                for c1, c2 in colors:
                    at_a = {i: component(left, c1, i, c2) for i in half}
                    at_b = {j: component(right, c1, j, c2) for j in {j for _, j in pairs}}
                    a = {i: (parts[0, n], parts[1, n], parts[2, n]) for i, n in at_a.items()}
                    b = {j: (parts[0, n], parts[2, n], parts[3, n]) for j, n in at_b.items()}
                    for i, j in pairs:
                        new = (a[i][2] * b[j][0], a[i][0] * b[j][1], a[i][1] * b[j][2])
                        old = sums.get((i, j))
                        sums[i, j] = new if old is None else tuple(o + v for o, v in zip(old, new))
                    for i in diagonal:
                        new = a[i][0] * a[i][0] + a[i][1] * a[i][1]
                        old = sums.get(i)
                        sums[i] = new if old is None else old + new
                for i, j in pairs:
                    first, second, third = sums[i, j]
                    put((left, i, right, j, 0), first - third)
                    put((left, i, right, j, 1), first - second)
                for i in diagonal:
                    put((left, i, right, i, 2), sums[i])


def front_kernel(
    grid_x, grid_y, prop, table_in, rows_in, dft_in, out,
    staged, parts, prod, dens, weights, sent, table, rows, dft,
    load_sems, small_sems, send_sem, recv_sem,
):
    devices, steps = out.shape[0], out.shape[1]
    tiles = staged.shape[0]
    entries = parts.shape[1]
    channels = table.shape[1]

    def load(t):
        return pltpu.make_async_copy(
            prop.at[:, :, pl.ds(t * LANES, LANES)], staged.at[t], load_sems.at[t]
        )

    me_x, me_y = lax.axis_index("gx"), lax.axis_index("gy")
    me = me_x * grid_y + me_y
    if grid_y == 4:
        columns_y = [lax.rem(me_y + 2, 4), 3 - me_y, me_y + 1 - 2 * lax.rem(me_y, 2)]
    else:
        columns_y = [lax.rem(me_y + i, grid_y) for i in range(1, grid_y)]

    def for_others(act):
        @pl.loop(0, grid_x)
        def _(i):
            to_x = lax.rem(me_x + i, grid_x)
            for to_y in columns_y:
                act(to_x, to_y)

        @pl.loop(1, grid_x)
        def _(i):
            act(lax.rem(me_x + i, grid_x), me_y)

    small = [
        pltpu.make_async_copy(source, target, small_sems.at[n])
        for n, (source, target) in enumerate(((table_in, table), (rows_in, rows), (dft_in, dft)))
    ]
    load(0).start()
    for copy in small:
        copy.start()
    for t in range(1, tiles):
        load(t).start()
    barrier = pltpu.get_barrier_semaphore()
    for_others(
        lambda x, y: pl.semaphore_signal(
            barrier, inc=1, device_id={"gx": x, "gy": y}, device_id_type=MESH
        )
    )
    small[0].wait()
    small[1].wait()
    weights[...] = folded_weights(jnp.transpose(table[...]), rows[...])
    small[2].wait()
    pl.semaphore_wait(barrier, grid_x * grid_y - 1)

    @pl.loop(0, steps)
    def _(k):
        @pl.loop(0, PAIRED)
        def _(half):
            t = k * PAIRED + half
            pltpu.make_async_copy(
                prop.at[:, :, pl.ds(0, LANES)], staged.at[t], load_sems.at[t]
            ).wait()
            real = staged[t, 0:entries].astype(jnp.float32)
            parts[0] = real
            imag = staged[t, entries : 2 * entries].astype(jnp.float32)
            parts[1] = imag
            parts[2] = real + imag
            parts[3] = real - imag
            products(parts, prod)
            for x in range(8):
                columns = prod[pl.ds(x, len(ROWS), stride=8), :].astype(jnp.bfloat16)
                value = jnp.dot(weights[...], columns, preferred_element_type=jnp.float32)
                dens[half, 0, pl.ds(x, channels, stride=8), :] = value[:channels]
                dens[half, 1, pl.ds(x, channels, stride=8), :] = value[channels:]

        pieces = []
        for half in range(PAIRED):
            left = jnp.concatenate([dens[half, 0], dens[half, 1]], axis=1).astype(jnp.bfloat16)
            value = lax.dot_general(
                dft[...], left, (((1,), (1,)), ((), ())), preferred_element_type=jnp.float32
            )
            pieces.append(value.reshape(devices, 2 * LANES // devices, LANES))
        block = jnp.concatenate(pieces, axis=1).astype(jnp.bfloat16)
        sent[:, k] = block
        pltpu.make_async_copy(sent.at[me, k], out.at[me, k], recv_sem).start()
        for_others(
            lambda x, y: pltpu.make_async_remote_copy(
                src_ref=sent.at[x * grid_y + y, k], dst_ref=out.at[me, k],
                send_sem=send_sem, recv_sem=recv_sem,
                device_id={"gx": x, "gy": y}, device_id_type=MESH,
            ).start()
        )

    pltpu.make_async_copy(out, out, recv_sem).wait()
    rest = sent.at[pl.ds(0, devices - 1)]
    pltpu.make_async_copy(rest, rest, send_sem).wait()


def front(prop, gamma_table, devices, grid_y, extent):
    entries, rows_x, sites = prop.shape
    tiles = sites // LANES
    steps = tiles // PAIRED
    height = 2 * LANES // devices * PAIRED
    channels = gamma_table.shape[0]
    rows = np.zeros((8, len(ROWS)), np.int32)
    rows[:5] = np.array(ROWS, np.int32).T
    return pl.pallas_call(
        functools.partial(front_kernel, devices // grid_y, grid_y),
        out_shape=jax.ShapeDtypeStruct((devices, steps, height, LANES), jnp.bfloat16),
        in_specs=[pl.BlockSpec(memory_space=pl.ANY)] * 4,
        out_specs=pl.BlockSpec(memory_space=pl.ANY),
        scratch_shapes=[
            pltpu.VMEM((tiles, entries, rows_x, LANES), jnp.bfloat16),
            pltpu.VMEM((4, entries // 2, rows_x, LANES), jnp.float32),
            pltpu.VMEM((len(ROWS) * rows_x, LANES), jnp.float32),
            pltpu.VMEM((PAIRED, 2, channels * rows_x, LANES), jnp.float32),
            pltpu.VMEM((2 * channels, len(ROWS)), jnp.bfloat16),
            pltpu.VMEM((devices, steps, height, LANES), jnp.bfloat16),
            pltpu.VMEM(gamma_table.shape[::-1], jnp.int32),
            pltpu.VMEM(rows.shape, jnp.int32),
            pltpu.VMEM((2 * LANES, 2 * LANES), jnp.bfloat16),
            pltpu.SemaphoreType.DMA((tiles,)),
            pltpu.SemaphoreType.DMA((3,)),
            pltpu.SemaphoreType.DMA,
            pltpu.SemaphoreType.DMA,
        ],
        compiler_params=pltpu.CompilerParams(
            vmem_limit_bytes=62 * 1024 * 1024, collective_id=0, has_side_effects=True
        ),
    )(prop, gamma_table.T, jnp.asarray(rows), jnp.asarray(table_z(extent), jnp.bfloat16))


def back_kernel(blocks_in, along_y, along_x, out, blocks, mid, sems):
    grid_x, _, width = blocks.shape
    copies = [
        pltpu.make_async_copy(blocks_in.at[gx], blocks.at[gx], sems.at[gx])
        for gx in range(grid_x)
    ]
    for copy in copies:
        copy.start()
    channels, local_k, extent, lanes = out.shape
    rows_x = width // channels
    cols = local_k * lanes
    for gx in range(grid_x):
        copies[gx].wait()
        mid[gx] = lax.dot_general(
            blocks[gx], along_y[...], (((0,), (0,)), ((), ())), preferred_element_type=jnp.float32
        )
    for g in range(channels):
        value = mid[:, g * rows_x : (g + 1) * rows_x, :].reshape(grid_x * rows_x, 2 * cols)
        value = value.astype(jnp.bfloat16)
        stacked = jnp.concatenate([value[:, :cols], value[:, cols:]], axis=0)
        result = jnp.dot(along_x[...], stacked, preferred_element_type=jnp.float32)
        for k in range(local_k):
            out[g, k] = result[:, k * lanes : (k + 1) * lanes]


def back(blocks, channels, extent, local_k):
    grid_x, _, width = blocks.shape
    vmem = pl.BlockSpec(memory_space=pltpu.VMEM)
    return pl.pallas_call(
        back_kernel,
        out_shape=jax.ShapeDtypeStruct((channels, local_k, extent, 2 * extent), jnp.float32),
        in_specs=[pl.BlockSpec(memory_space=pl.ANY), vmem, vmem],
        out_specs=vmem,
        scratch_shapes=[
            pltpu.VMEM(blocks.shape, blocks.dtype),
            pltpu.VMEM((grid_x, width, 4 * local_k * extent), jnp.float32),
            pltpu.SemaphoreType.DMA((grid_x,)),
        ],
        compiler_params=pltpu.CompilerParams(vmem_limit_bytes=62 * 1024 * 1024),
    )(
        blocks,
        jnp.asarray(table_y(extent, local_k), jnp.bfloat16),
        jnp.asarray(table_x(extent), jnp.bfloat16),
    )


def body(propagator, gamma_table):
    slices, rows_x, sites = propagator.shape[0], propagator.shape[-2], propagator.shape[-1]
    grid_x, grid_y = lax.axis_size("gx"), lax.axis_size("gy")
    devices = grid_x * grid_y
    extent = grid_x * rows_x
    channels = gamma_table.shape[0]
    local_k = extent // devices
    results = []
    for t in range(slices):
        prop = propagator[t].reshape(-1, rows_x, sites)
        blocks = front(prop, gamma_table, devices, grid_y, extent)
        blocks = blocks.reshape(grid_x, -1, LANES)
        results.append(back(blocks, channels, extent, local_k))
    return jnp.stack(results)


def solution(mesh):
    return jax.shard_map(
        body,
        mesh=mesh,
        in_specs=(P("ta", None, None, None, None, None, "gx", "gy"), P()),
        out_specs=P("ta", None, ("gx", "gy"), None, None),
        check_vma=False,
    )
```

```python
import functools
import math

import jax
import jax.numpy as jnp
import numpy as np
from jax import lax
from jax.experimental import pallas as pl
from jax.experimental.pallas import tpu as pltpu
from jax.sharding import PartitionSpec as P

LANES = 128
SPINS = 4
COLORS = 3
PAIRED = 2
MESH = pl.DeviceIdType.MESH


def pair_rows():
    rows = []
    for left in range(SPINS):
        for right in range(left, SPINS):
            for i in range(SPINS):
                for j in range(SPINS):
                    if left == right and i > j:
                        continue
                    if left == right and i == j:
                        rows.append((left, i, right, j, 2))
                    else:
                        rows.append((left, i, right, j, 0))
                        rows.append((left, i, right, j, 1))
    return rows


ROWS = pair_rows()
ROW_OF = {row: position for position, row in enumerate(ROWS)}


def dft_tables(length):
    index = np.arange(length)
    angles = (index[:, None] * index[None, :] % length) * (2.0 * math.pi / length)
    norm = 1.0 / math.sqrt(length)
    half = lambda v: (v * norm).astype(jnp.bfloat16).astype(np.float32)
    return half(np.cos(angles)), half(np.sin(angles))


def table_z(extent):
    cosine, sine = dft_tables(extent)
    per_tile = LANES // extent
    same = np.eye(per_tile, dtype=np.float32)
    block = np.zeros((extent, 2, per_tile, 2, per_tile, extent), np.float32)
    for c_out, c_in, values in ((0, 0, cosine), (0, 1, sine), (1, 0, -sine), (1, 1, cosine)):
        block[:, c_out, :, c_in] = np.einsum("zk,ab->kabz", values, same)
    return block.reshape(2 * LANES, 2 * LANES)


def table_y(extent, local_k):
    cosine, sine = dft_tables(extent)
    per_tile = LANES // extent
    groups = extent // per_tile
    block = np.zeros((groups, local_k, 2, per_tile, 2, local_k, 2, extent), np.float32)
    entries = (
        (0, 0, 0, cosine), (0, 0, 1, sine), (0, 1, 0, -sine), (0, 1, 1, cosine),
        (1, 0, 0, -sine), (1, 0, 1, cosine), (1, 1, 0, -cosine), (1, 1, 1, -sine),
    )
    for copy, c_out, c_in, values in entries:
        for k in range(local_k):
            block[:, k, c_in, :, copy, k, c_out] = values.reshape(groups, per_tile, extent)
    return block.reshape(groups * local_k * 2 * per_tile, 2 * local_k * 2 * extent)


def table_x(extent):
    cosine, sine = dft_tables(extent)
    return np.concatenate([cosine.T, sine.T], axis=1)


def folded_weights(table, rows):
    channels = table.shape[0]
    a1, a2, b1, b2, kind = (rows[i : i + 1, :] for i in range(5))

    def pick(spin, base):
        value = jnp.zeros((channels, rows.shape[1]), jnp.int32)
        for s in range(SPINS):
            value = jnp.where(spin == s, table[:, base + s : base + s + 1], value)
        return value

    def term(l1, l2, r1, r2):
        hit = (pick(r1, 0) == l1) & (pick(l2, 0) == r2)
        code = (pick(r1, SPINS) + pick(l2, SPINS)) & 3
        one = jnp.where(hit, 1.0, 0.0)
        real = jnp.where(code == 0, one, jnp.where(code == 2, -one, 0.0))
        imag = jnp.where(code == 1, one, jnp.where(code == 3, -one, 0.0))
        return real, imag

    fore_real, fore_imag = term(a1, a2, b1, b2)
    back_real, back_imag = term(b1, b2, a1, a2)
    sign = jnp.where(kind == 0, 1.0, jnp.where(kind == 1, -1.0, 0.0))
    real = fore_real + sign * back_real
    imag = fore_imag + sign * back_imag
    weight_real = jnp.where(kind == 1, -imag, real)
    weight_imag = jnp.where(kind == 1, real, imag)
    return jnp.concatenate([weight_real, weight_imag], axis=0).astype(jnp.bfloat16)


def component(s1, c1, s2, c2):
    return ((s1 * COLORS + c1) * SPINS + s2) * COLORS + c2


def products(parts, rows_out):
    def put(row, value):
        rows_out[pl.ds(ROW_OF[row] * 8, 8), :] = value

    colors = [(c1, c2) for c1 in range(COLORS) for c2 in range(COLORS)]
    for left in range(SPINS):
        for right in range(left, SPINS):
            for half in ((0, 1), (2, 3)):
                pairs = [(i, j) for i in half for j in range(SPINS) if left != right or i < j]
                diagonal = half if left == right else ()
                sums = {}
                for c1, c2 in colors:
                    at_a = {i: component(left, c1, i, c2) for i in half}
                    at_b = {j: component(right, c1, j, c2) for j in {j for _, j in pairs}}
                    a = {i: (parts[0, n], parts[1, n], parts[2, n]) for i, n in at_a.items()}
                    b = {j: (parts[0, n], parts[2, n], parts[3, n]) for j, n in at_b.items()}
                    for i, j in pairs:
                        new = (a[i][2] * b[j][0], a[i][0] * b[j][1], a[i][1] * b[j][2])
                        old = sums.get((i, j))
                        sums[i, j] = new if old is None else tuple(o + v for o, v in zip(old, new))
                    for i in diagonal:
                        new = a[i][0] * a[i][0] + a[i][1] * a[i][1]
                        old = sums.get(i)
                        sums[i] = new if old is None else old + new
                for i, j in pairs:
                    first, second, third = sums[i, j]
                    put((left, i, right, j, 0), first - third)
                    put((left, i, right, j, 1), first - second)
                for i in diagonal:
                    put((left, i, right, i, 2), sums[i])


def front_kernel(
    grid_x, grid_y, prop, table_in, rows_in, dft_in, out,
    staged, parts, prod, dens, weights, sent, table, rows, dft,
    load_sems, small_sems, send_sem, recv_sem,
):
    devices, steps = out.shape[0], out.shape[1]
    tiles = staged.shape[0]
    entries = parts.shape[1]
    channels = table.shape[1]

    def load(t):
        return pltpu.make_async_copy(
            prop.at[:, :, pl.ds(t * LANES, LANES)], staged.at[t], load_sems.at[t]
        )

    me_x, me_y = lax.axis_index("gx"), lax.axis_index("gy")
    me = me_x * grid_y + me_y
    if grid_y == 4:
        columns_y = [lax.rem(me_y + 2, 4), me_y + 1 - 2 * lax.rem(me_y, 2), 3 - me_y]
    else:
        columns_y = [lax.rem(me_y + i, grid_y) for i in range(1, grid_y)]

    def for_others(act):
        @pl.loop(1, grid_x)
        def _(i):
            to_x = lax.rem(me_x + i, grid_x)
            for to_y in columns_y:
                act(to_x, to_y)
            act(to_x, me_y)

        for to_y in columns_y:
            act(me_x, to_y)

    small = [
        pltpu.make_async_copy(source, target, small_sems.at[n])
        for n, (source, target) in enumerate(((table_in, table), (rows_in, rows), (dft_in, dft)))
    ]
    load(0).start()
    for copy in small:
        copy.start()
    for t in range(1, tiles):
        load(t).start()
    barrier = pltpu.get_barrier_semaphore()
    for_others(
        lambda x, y: pl.semaphore_signal(
            barrier, inc=1, device_id={"gx": x, "gy": y}, device_id_type=MESH
        )
    )
    small[0].wait()
    small[1].wait()
    weights[...] = folded_weights(jnp.transpose(table[...]), rows[...])
    small[2].wait()
    pl.semaphore_wait(barrier, grid_x * grid_y - 1)

    @pl.loop(0, steps)
    def _(k):
        @pl.loop(0, PAIRED)
        def _(half):
            t = k * PAIRED + half
            pltpu.make_async_copy(
                prop.at[:, :, pl.ds(0, LANES)], staged.at[t], load_sems.at[t]
            ).wait()
            real = staged[t, 0:entries].astype(jnp.float32)
            parts[0] = real
            imag = staged[t, entries : 2 * entries].astype(jnp.float32)
            parts[1] = imag
            parts[2] = real + imag
            parts[3] = real - imag
            products(parts, prod)
            for x in range(8):
                columns = prod[pl.ds(x, len(ROWS), stride=8), :].astype(jnp.bfloat16)
                value = jnp.dot(weights[...], columns, preferred_element_type=jnp.float32)
                dens[half, 0, pl.ds(x, channels, stride=8), :] = value[:channels]
                dens[half, 1, pl.ds(x, channels, stride=8), :] = value[channels:]

        pieces = []
        for half in range(PAIRED):
            left = jnp.concatenate([dens[half, 0], dens[half, 1]], axis=1).astype(jnp.bfloat16)
            value = lax.dot_general(
                dft[...], left, (((1,), (1,)), ((), ())), preferred_element_type=jnp.float32
            )
            pieces.append(value.reshape(devices, 2 * LANES // devices, LANES))
        block = jnp.concatenate(pieces, axis=1).astype(jnp.bfloat16)
        sent[:, k] = block
        pltpu.make_async_copy(sent.at[me, k], out.at[me, k], recv_sem).start()
        for_others(
            lambda x, y: pltpu.make_async_remote_copy(
                src_ref=sent.at[x * grid_y + y, k], dst_ref=out.at[me, k],
                send_sem=send_sem, recv_sem=recv_sem,
                device_id={"gx": x, "gy": y}, device_id_type=MESH,
            ).start()
        )

    pltpu.make_async_copy(out, out, recv_sem).wait()
    rest = sent.at[pl.ds(0, devices - 1)]
    pltpu.make_async_copy(rest, rest, send_sem).wait()


def front(prop, gamma_table, devices, grid_y, extent):
    entries, rows_x, sites = prop.shape
    tiles = sites // LANES
    steps = tiles // PAIRED
    height = 2 * LANES // devices * PAIRED
    channels = gamma_table.shape[0]
    rows = np.zeros((8, len(ROWS)), np.int32)
    rows[:5] = np.array(ROWS, np.int32).T
    return pl.pallas_call(
        functools.partial(front_kernel, devices // grid_y, grid_y),
        out_shape=jax.ShapeDtypeStruct((devices, steps, height, LANES), jnp.bfloat16),
        in_specs=[pl.BlockSpec(memory_space=pl.ANY)] * 4,
        out_specs=pl.BlockSpec(memory_space=pl.ANY),
        scratch_shapes=[
            pltpu.VMEM((tiles, entries, rows_x, LANES), jnp.bfloat16),
            pltpu.VMEM((4, entries // 2, rows_x, LANES), jnp.float32),
            pltpu.VMEM((len(ROWS) * rows_x, LANES), jnp.float32),
            pltpu.VMEM((PAIRED, 2, channels * rows_x, LANES), jnp.float32),
            pltpu.VMEM((2 * channels, len(ROWS)), jnp.bfloat16),
            pltpu.VMEM((devices, steps, height, LANES), jnp.bfloat16),
            pltpu.VMEM(gamma_table.shape[::-1], jnp.int32),
            pltpu.VMEM(rows.shape, jnp.int32),
            pltpu.VMEM((2 * LANES, 2 * LANES), jnp.bfloat16),
            pltpu.SemaphoreType.DMA((tiles,)),
            pltpu.SemaphoreType.DMA((3,)),
            pltpu.SemaphoreType.DMA,
            pltpu.SemaphoreType.DMA,
        ],
        compiler_params=pltpu.CompilerParams(
            vmem_limit_bytes=62 * 1024 * 1024, collective_id=0, has_side_effects=True
        ),
    )(prop, gamma_table.T, jnp.asarray(rows), jnp.asarray(table_z(extent), jnp.bfloat16))


def back_kernel(blocks, along_y, along_x, out, mid):
    grid_x, _, width = blocks.shape
    channels, local_k, extent, lanes = out.shape
    rows_x = width // channels
    cols = local_k * lanes
    for gx in range(grid_x):
        mid[gx] = lax.dot_general(
            blocks[gx], along_y[...], (((0,), (0,)), ((), ())), preferred_element_type=jnp.float32
        )
    for g in range(channels):
        value = mid[:, g * rows_x : (g + 1) * rows_x, :].reshape(grid_x * rows_x, 2 * cols)
        value = value.astype(jnp.bfloat16)
        stacked = jnp.concatenate([value[:, :cols], value[:, cols:]], axis=0)
        result = jnp.dot(along_x[...], stacked, preferred_element_type=jnp.float32)
        for k in range(local_k):
            out[g, k] = result[:, k * lanes : (k + 1) * lanes]


def back(blocks, channels, extent, local_k):
    grid_x, _, width = blocks.shape
    vmem = pl.BlockSpec(memory_space=pltpu.VMEM)
    return pl.pallas_call(
        back_kernel,
        out_shape=jax.ShapeDtypeStruct((channels, local_k, extent, 2 * extent), jnp.float32),
        in_specs=[vmem] * 3,
        out_specs=vmem,
        scratch_shapes=[pltpu.VMEM((grid_x, width, 4 * local_k * extent), jnp.float32)],
        compiler_params=pltpu.CompilerParams(vmem_limit_bytes=24 * 1024 * 1024),
    )(
        blocks,
        jnp.asarray(table_y(extent, local_k), jnp.bfloat16),
        jnp.asarray(table_x(extent), jnp.bfloat16),
    )


def body(propagator, gamma_table):
    slices, rows_x, sites = propagator.shape[0], propagator.shape[-2], propagator.shape[-1]
    grid_x, grid_y = lax.axis_size("gx"), lax.axis_size("gy")
    devices = grid_x * grid_y
    extent = grid_x * rows_x
    channels = gamma_table.shape[0]
    local_k = extent // devices
    results = []
    for t in range(slices):
        prop = propagator[t].reshape(-1, rows_x, sites)
        blocks = front(prop, gamma_table, devices, grid_y, extent)
        blocks = blocks.reshape(grid_x, -1, LANES)
        results.append(back(blocks, channels, extent, local_k))
    return jnp.stack(results)


def solution(mesh):
    return jax.shard_map(
        body,
        mesh=mesh,
        in_specs=(P("ta", None, None, None, None, None, "gx", "gy"), P()),
        out_specs=P("ta", None, ("gx", "gy"), None, None),
        check_vma=False,
    )
```
